32 devices in a mesh: gx: 4 (over x, core), gy: 8 (over z, y).
Axes of the slice: x: 2, y: 2, z: 4, core: 2. Of those that a mesh axis runs over, the one named last changes fastest.
Arguments:
- activations: bfloat16 [4096, 8192], P('gx', 'gy'), may hold values from -12 to 12
- out_grads: bfloat16 [4096, 4096], P('gx', 'gy'), may hold values from -12 to 12
- left_roots: float32 [32, 1024, 1024], P(('gx', 'gy')), may hold values from -20 to 20, as said below
- right_roots: float32 [32, 1024, 1024], P(('gx', 'gy')), may hold values from -20 to 20, as said below
Outputs:
- update: bfloat16 [8192, 4096], P(None, 'gy')
The draws below stay inside these ranges and needn't reach their ends.
Inputs may be any that keep to these rules, and one draw needn't show every extreme that they name: `left_roots`: each block is symmetric positive definite. `right_roots`: each block is symmetric positive definite.
All inputs are finite; a program needn't handle non-finite values.
Results may differ from the reference program's by a relative error of at most 0.001.
Values may be sent and summed in bfloat16 or wider, within the bound.
No kernel may reach another device: no remote copies, remote signals or barrier semaphores. Data moves between devices by JAX's collectives and lax.ppermute only.
A program may use at most 128 MiB of HBM per device.

```python
import math
import jax
import jax.numpy as jnp
from jax import lax

D = 8192
BLK = 1024
TOKENS = 4096
COLS = 4096
NBLK = 32
N_GY = 8


def scaled_draw(key, row_count, width):
    key_scale, key_noise = jax.random.split(key, 2)
    feature_scale = jnp.exp(jax.random.uniform(key_scale, (width,), jnp.float32, math.log(0.3), math.log(3.0)))
    values = jax.random.normal(key_noise, (row_count, width), jnp.float32) * feature_scale[None, :]
    return jnp.clip(values, -12.0, 12.0).astype(jnp.bfloat16)


def draw_activations(key, part):
    return scaled_draw(jax.random.fold_in(key, 11), TOKENS, D)


def draw_out_grads(key, part):
    return scaled_draw(jax.random.fold_in(key, 23), TOKENS, COLS)


def root_draw(key, salt):
    base = jax.random.fold_in(key, salt)

    def single(index):
        sub = jax.random.fold_in(base, index)
        key_scale, key_noise = jax.random.split(sub)
        scales = jnp.exp(jax.random.uniform(key_scale, (BLK,), jnp.float32, math.log(0.3), math.log(3.0)))
        noise = jax.random.normal(key_noise, (BLK, BLK), jnp.float32)
        symmetric = (noise + noise.T) * (0.4 / math.sqrt(2.0 * BLK))
        core = jnp.eye(BLK, dtype=jnp.float32) + symmetric
        return scales[:, None] * core * scales[None, :]
    return lax.map(single, jnp.arange(NBLK, dtype=jnp.int32))


def draw_left_roots(key, part):
    return root_draw(key, 37)


def draw_right_roots(key, part):
    return root_draw(key, 41)


def setup_inputs(seed: int = 0) -> dict:
    splits = jax.random.split(jax.random.key(seed), 5)
    activations = draw_activations(jax.random.fold_in(splits[4], 71), 0)
    out_grads = draw_out_grads(jax.random.fold_in(splits[4], 71), 0)
    left_roots = draw_left_roots(jax.random.fold_in(splits[4], 71), 0)
    right_roots = draw_right_roots(jax.random.fold_in(splits[4], 71), 0)
    return dict(activations=activations, out_grads=out_grads, left_roots=left_roots, right_roots=right_roots)


epsilon = 1e-06

def precondition(items):
    grad_block, left_root, right_root = items
    shaped = jnp.dot(jnp.dot(left_root, grad_block, precision=lax.Precision.HIGHEST), right_root, precision=lax.Precision.HIGHEST)
    graft = jnp.sqrt(jnp.mean(grad_block * grad_block) + epsilon) / jnp.sqrt(jnp.mean(shaped * shaped) + epsilon)
    return (shaped * graft).astype(jnp.bfloat16)

def reference(activations, out_grads, left_roots, right_roots):
    weight_grad = lax.dot_general(activations, out_grads, (((0,), (0,)), ((), ())), preferred_element_type=jnp.float32)
    row_blocks = D // BLK
    col_blocks = COLS // BLK
    tiles = weight_grad.reshape(row_blocks, BLK, col_blocks, BLK).transpose(0, 2, 1, 3)
    number = jnp.arange(NBLK, dtype=jnp.int32)
    row_of = (2 * (number // N_GY) + number % 2).astype(jnp.int32)
    col_of = (number % N_GY // 2).astype(jnp.int32)
    grad_blocks = tiles[row_of, col_of]
    updates = lax.map(precondition, (grad_blocks, left_roots, right_roots))
    grid_rows = jnp.arange(row_blocks, dtype=jnp.int32)[:, None]
    grid_cols = jnp.arange(col_blocks, dtype=jnp.int32)[None, :]
    owner = (grid_rows // 2 * N_GY + 2 * grid_cols + grid_rows % 2).astype(jnp.int32)
    placed = updates[owner]
    return placed.transpose(0, 2, 1, 3).reshape(D, COLS)
```

```python
import jax
import jax.numpy as jnp
from jax import lax
from jax.sharding import PartitionSpec as P

epsilon = 1e-06
AXES = ("gx", "gy")
SPLIT = 2


def partner(block, axis, distance):
    count = lax.axis_size(axis)
    route = []
    for low in range(count):
        high = low | 1 << distance
        if high != low and high < count:
            route += [(low, high), (high, low)]
    return lax.ppermute(block, axis, route)


def general(activations, out_grads, left_roots, right_roots):
    block_size = left_roots.shape[1]
    half_width = block_size // 2
    parity = lax.axis_index("gy") % 2
    is_even = parity == 0
    gathered = lax.all_gather(activations, "gy", axis=1, tiled=True)
    summed = lax.psum_scatter(
        lax.dot_general(
            gathered, out_grads, (((0,), (0,)), ((), ())), preferred_element_type=jnp.float32
        ),
        "gx",
        scatter_dimension=0,
        tiled=True,
    )
    own_part = lax.dynamic_slice_in_dim(summed, parity * block_size, block_size, 0)
    far_part = lax.dynamic_slice_in_dim(summed, (1 - parity) * block_size, block_size, 0)
    received = partner(far_part, "gy", 0)
    left_block = jnp.where(is_even, own_part, received)
    right_block = jnp.where(is_even, received, own_part)
    grad_block = jnp.concatenate([left_block, right_block], axis=1)
    finished = precondition(grad_block, left_roots[0], right_roots[0])
    own_part = lax.dynamic_slice_in_dim(finished, parity * half_width, half_width, 1)
    far_part = lax.dynamic_slice_in_dim(finished, (1 - parity) * half_width, half_width, 1)
    received = partner(far_part, "gy", 0)
    upper_rows = jnp.where(is_even, own_part, received)
    lower_rows = jnp.where(is_even, received, own_part)
    paired = jnp.concatenate([upper_rows, lower_rows], axis=0)
    return lax.all_gather(paired, "gx", axis=0, tiled=True)


def precondition(grad_block, left_root, right_root):
    shaped = jnp.dot(
        jnp.dot(left_root, grad_block, precision=lax.Precision.HIGH),
        right_root,
        precision=lax.Precision.HIGH,
    )
    graft = jnp.sqrt(jnp.mean(grad_block * grad_block) + epsilon) / jnp.sqrt(
        jnp.mean(shaped * shaped) + epsilon
    )
    return (shaped * graft).astype(jnp.bfloat16)


def routes(n_gx, n_gy, target):
    found = []
    for gx in range(n_gx):
        for gy in range(n_gy):
            to = target(gx // 2, gx % 2, gy // 2, gy % 2)
            if to is not None:
                x, core, z, y = to
                found.append((gx * n_gy + gy, (2 * x + core) * n_gy + 2 * z + y))
    return found


def send(block, route):
    return lax.ppermute(block, AXES, route)


def chosen(table, z):
    value = jnp.int32(table[0])
    for position in range(1, len(table)):
        value = jnp.where(z == position, jnp.int32(table[position]), value)
    return value


def lined(activations, out_grads, left_roots, right_roots):
    n_gx, n_gy = lax.axis_size("gx"), lax.axis_size("gy")
    n_z = n_gy // 2
    gx, gy = lax.axis_index("gx"), lax.axis_index("gy")
    x, core, z, y = gx // 2, gx % 2, gy // 2, gy % 2
    block_size = left_roots.shape[1]
    half = block_size // 2
    piece = half // SPLIT

    def route(target):
        return routes(n_gx, n_gy, target)

    across_x = route(lambda x, c, z, y: (1 - x, c, z, y))
    across_y = route(lambda x, c, z, y: (x, c, z, 1 - y))
    across_xy = route(lambda x, c, z, y: (1 - x, c, z, 1 - y))
    across_cores = route(lambda x, c, z, y: (x, 1 - c, z, y))

    own = []
    for h in range(SPLIT):
        near = lax.dynamic_slice_in_dim(activations, core * half + h * piece, piece, 1)
        far = lax.dynamic_slice_in_dim(activations, (1 - core) * half + h * piece, piece, 1)
        own.append(jnp.concatenate([near, send(far, across_cores)], axis=0))

    up_1 = route(lambda x, c, z, y: (x, c, z + 1, y) if z < n_z - 1 else None)
    down_1 = route(lambda x, c, z, y: (x, c, z - 1, y) if z > 0 else None)
    up_2 = route(lambda x, c, z, y: (x, c, z + 1, y) if 0 < z < n_z - 1 else None)
    down_2 = route(lambda x, c, z, y: (x, c, z - 1, y) if 0 < z < n_z - 1 else None)
    ends = route(
        lambda x, c, z, y: (x, c, z + 1, y) if z == n_z - 2 else ((x, c, z - 1, y) if z == 1 else None)
    )
    is_upper = z >= n_z // 2
    is_end = (z == 0) | (z == n_z - 1)
    first_up = [send(a, up_1) for a in own]
    first_down = [send(a, down_1) for a in own]
    second_up = [send(a, up_2) for a in first_up]
    second_down = [send(a, down_2) for a in first_down]
    second = [jnp.where(is_upper, u, d) for u, d in zip(second_up, second_down)]
    third = [send(a, ends) for a in second]
    nearest = [jnp.where(is_upper, u, d) for u, d in zip(first_up, first_down)]
    opposite = [jnp.where(is_upper, d, u) for u, d in zip(first_up, first_down)]
    rounds = [
        (own, [0, 1, 2, 3]),
        (nearest, [1, 2, 1, 2]),
        ([jnp.where(is_end, s, o) for s, o in zip(second, opposite)], [2, 0, 3, 1]),
        ([jnp.where(is_end, t, s) for t, s in zip(third, second)], [3, 3, 0, 0]),
    ]

    other_half = send(out_grads, across_y)
    columns = jnp.where(
        y == 0,
        jnp.concatenate([out_grads, other_half], axis=1),
        jnp.concatenate([other_half, out_grads], axis=1),
    )
    columns = jnp.concatenate([columns, send(columns, across_cores)], axis=0)

    mine = [None] * SPLIT
    theirs = [None] * SPLIT
    for chunk, table in rounds:
        source = chosen(table, z)

        def to_owner(x, c, z, y):
            owner = table[z] // 2
            return (owner, c, z, y) if x != owner else None

        for h in range(SPLIT):
            partial = lax.dot_general(
                chunk[h], columns, (((0,), (0,)), ((), ())), preferred_element_type=jnp.float32
            )
            total = partial + send(partial, route(to_owner))
            if mine[h] is None:
                mine[h], theirs[h] = total, total
            else:
                mine[h] = jnp.where(source == gx, total, mine[h])
                theirs[h] = jnp.where(source == 2 * x + 1 - core, total, theirs[h])
    theirs = [send(t, across_cores) for t in theirs]
    mine = jnp.concatenate(mine, axis=0)
    theirs = jnp.concatenate(theirs, axis=0)
    grad_block = jnp.concatenate(
        [jnp.where(core == 0, mine, theirs), jnp.where(core == 0, theirs, mine)], axis=0
    )
    finished = precondition(grad_block, left_roots[0], right_roots[0])

    near = lax.dynamic_slice_in_dim(finished, y * half, half, 1)
    far = lax.dynamic_slice_in_dim(finished, (1 - y) * half, half, 1)
    parts = [
        (near, x, y),
        (send(near, across_x), 1 - x, y),
        (send(far, across_y), x, 1 - y),
        (send(far, across_xy), 1 - x, 1 - y),
    ]
    result = jnp.zeros((n_gx * 2 * block_size, half), jnp.bfloat16)
    for part, from_x, from_y in parts:
        other = send(part, across_cores)
        for block, from_core in ((part, core), (other, 1 - core)):
            row = (4 * from_x + 2 * from_core + from_y) * block_size
            result = lax.dynamic_update_slice(result, block, (row, jnp.int32(0)))
    return result


def solution(mesh):
    in_specs = (
        P("gx", "gy"),
        P("gx", "gy"),
        P(("gx", "gy"), None, None),
        P(("gx", "gy"), None, None),
    )
    out_specs = P(None, "gy")

    def local(activations, out_grads, left_roots, right_roots):
        n_gx, n_gy = lax.axis_size("gx"), lax.axis_size("gy")
        same = activations.shape[1] == left_roots.shape[1]
        form = lined if same and n_gx == 4 and n_gy == 2 * n_gx else general
        return form(activations, out_grads, left_roots, right_roots)

    return jax.shard_map(local, mesh=mesh, in_specs=in_specs, out_specs=out_specs, check_vma=False)
```

```python
import jax
import jax.numpy as jnp
from jax import lax
from jax.sharding import PartitionSpec as P


epsilon = 1e-06
AXES = ("gx", "gy")
PARTS = (1, 1)


def partner(block, axis, distance):
    count = lax.axis_size(axis)
    route = []
    for low in range(count):
        high = low | 1 << distance
        if high != low and high < count:
            route += [(low, high), (high, low)]
    return lax.ppermute(block, axis, route)


def general(activations, out_grads, left_roots, right_roots):
    block_size = left_roots.shape[1]
    half_width = block_size // 2
    parity = lax.axis_index("gy") % 2
    is_even = parity == 0
    gathered = lax.all_gather(activations, "gy", axis=1, tiled=True)
    summed = lax.psum_scatter(
        lax.dot_general(
            gathered, out_grads, (((0,), (0,)), ((), ())), preferred_element_type=jnp.float32
        ),
        "gx",
        scatter_dimension=0,
        tiled=True,
    )
    own_part = lax.dynamic_slice_in_dim(summed, parity * block_size, block_size, 0)
    far_part = lax.dynamic_slice_in_dim(summed, (1 - parity) * block_size, block_size, 0)
    received = partner(far_part, "gy", 0)
    left_block = jnp.where(is_even, own_part, received)
    right_block = jnp.where(is_even, received, own_part)
    grad_block = jnp.concatenate([left_block, right_block], axis=1)
    finished = precondition(grad_block, left_roots[0], right_roots[0])
    own_part = lax.dynamic_slice_in_dim(finished, parity * half_width, half_width, 1)
    far_part = lax.dynamic_slice_in_dim(finished, (1 - parity) * half_width, half_width, 1)
    received = partner(far_part, "gy", 0)
    upper_rows = jnp.where(is_even, own_part, received)
    lower_rows = jnp.where(is_even, received, own_part)
    paired = jnp.concatenate([upper_rows, lower_rows], axis=0)
    return lax.all_gather(paired, "gx", axis=0, tiled=True)


def precondition(grad_block, left_root, right_root):
    shaped = jnp.dot(
        jnp.dot(left_root, grad_block, precision=lax.Precision.HIGH),
        right_root,
        precision=lax.Precision.HIGH,
    )
    graft = jnp.sqrt(jnp.mean(grad_block * grad_block) + epsilon) / jnp.sqrt(
        jnp.mean(shaped * shaped) + epsilon
    )
    return (shaped * graft).astype(jnp.bfloat16)


def routes(n_gx, n_gy, target):
    found = []
    for gx in range(n_gx):
        for gy in range(n_gy):
            to = target(gx // 2, gx % 2, gy // 2, gy % 2)
            if to is not None:
                x, core, z, y = to
                found.append((gx * n_gy + gy, (2 * x + core) * n_gy + 2 * z + y))
    return found


def send(block, route):
    return lax.ppermute(block, AXES, route)


def chosen(table, z):
    value = jnp.int32(table[0])
    for position in range(1, len(table)):
        value = jnp.where(z == position, jnp.int32(table[position]), value)
    return value


def lined(activations, out_grads, left_roots, right_roots):
    n_gx, n_gy = lax.axis_size("gx"), lax.axis_size("gy")
    n_z = n_gy // 2
    gx, gy = lax.axis_index("gx"), lax.axis_index("gy")
    x, core, z, y = gx // 2, gx % 2, gy // 2, gy % 2
    block_size = left_roots.shape[1]
    half = block_size // 2
    widths = [half * part // sum(PARTS) for part in PARTS]
    starts = [sum(widths[:h]) for h in range(len(widths))]
    pieces = range(len(widths))
    left_root, right_root = left_roots[0], right_roots[0]

    def route(target):
        return routes(n_gx, n_gy, target)

    across_x = route(lambda x, c, z, y: (1 - x, c, z, y))
    across_y = route(lambda x, c, z, y: (x, c, z, 1 - y))
    across_xy = route(lambda x, c, z, y: (1 - x, c, z, 1 - y))
    across_cores = route(lambda x, c, z, y: (x, 1 - c, z, y))

    def moved(block, path):
        return send(block, path)

    own = []
    for h in pieces:
        near = lax.dynamic_slice_in_dim(activations, core * half + starts[h], widths[h], 1)
        far = lax.dynamic_slice_in_dim(
            activations, (1 - core) * half + starts[h], widths[h], 1
        )
        swapped = moved(far, across_cores)
        own.append(jnp.concatenate([near, swapped], axis=0))

    up_1 = route(lambda x, c, z, y: (x, c, z + 1, y) if z < n_z - 1 else None)
    down_1 = route(lambda x, c, z, y: (x, c, z - 1, y) if z > 0 else None)
    up_2 = route(lambda x, c, z, y: (x, c, z + 1, y) if 0 < z < n_z - 1 else None)
    down_2 = route(lambda x, c, z, y: (x, c, z - 1, y) if 0 < z < n_z - 1 else None)
    ends = route(
        lambda x, c, z, y: (x, c, z + 1, y) if z == n_z - 2 else ((x, c, z - 1, y) if z == 1 else None)
    )
    is_upper = z >= n_z // 2
    is_end = (z == 0) | (z == n_z - 1)
    first_up = [moved(own[h], up_1) for h in pieces]
    first_down = [moved(own[h], down_1) for h in pieces]
    second_up = [moved(first_up[h], up_2) for h in pieces]
    second_down = [moved(first_down[h], down_2) for h in pieces]
    second = [jnp.where(is_upper, u, d) for u, d in zip(second_up, second_down)]
    third = [moved(second[h], ends) for h in pieces]

    other_half = moved(out_grads, across_y)
    columns = jnp.where(
        y == 0,
        jnp.concatenate([out_grads, other_half], axis=1),
        jnp.concatenate([other_half, out_grads], axis=1),
    )
    columns = jnp.concatenate([columns, moved(columns, across_cores)], axis=0)

    def arrived(step, h):
        if step == 0:
            return own[h]
        if step == 1:
            return jnp.where(is_upper, first_up[h], first_down[h])
        if step == 2:
            opposite = jnp.where(is_upper, first_down[h], first_up[h])
            return jnp.where(is_end, second[h], opposite)
        return jnp.where(is_end, third[h], second[h])

    def partial_sum(step, h):
        return lax.dot_general(
            arrived(step, h),
            columns,
            (((0,), (0,)), ((), ())),
            preferred_element_type=jnp.float32,
        )

    tables = [[0, 1, 2, 3], [1, 2, 1, 2], [2, 0, 3, 1], [3, 3, 0, 0]]
    sources = [chosen(table, z) for table in tables]
    final = tables[-1]
    same_core = route(
        lambda x, c, z, y: (1 - x, c, z, y)
        if (x, c) == (1 - final[z] // 2, final[z] % 2)
        else None
    )
    cross_core = route(
        lambda x, c, z, y: (1 - x, 1 - c, z, y)
        if (x, c) == (1 - final[z] // 2, 1 - final[z] % 2)
        else None
    )
    chip_mate = route(
        lambda x, c, z, y: (x, 1 - c, z, y)
        if (x, c) == (final[z] // 2, 1 - final[z] % 2)
        else None
    )
    shaped = None
    squares = jnp.float32(0)
    for h in pieces:
        mine = theirs = None
        for step in range(3):
            part = partial_sum(step, h)
            table = tables[step]

            def to_owner(x, c, z, y):
                owner = table[z] // 2
                return (owner, c, z, y) if x != owner else None

            crossed = moved(part, route(to_owner))
            total = part + crossed
            if mine is None:
                mine, theirs = total, total
            else:
                mine = jnp.where(sources[step] == gx, total, mine)
                theirs = jnp.where(sources[step] == 2 * x + 1 - core, total, theirs)
        mine, theirs = lax.optimization_barrier((mine, theirs))
        theirs = moved(theirs, across_cores)
        part = partial_sum(3, h)
        from_same = moved(part, same_core)
        from_cross = moved(part, cross_core)
        from_mate = moved(part, chip_mate)
        low, high = starts[h], starts[h] + widths[h]
        weights = jnp.concatenate(
            [left_root[:, low:high], left_root[:, half + low : half + high]], axis=1
        )
        is_last = sources[3] == gx
        mine = jnp.where(is_last, part + from_same, mine)
        theirs = jnp.where(is_last, from_cross + from_mate, theirs)
        rows = jnp.concatenate(
            [jnp.where(core == 0, mine, theirs), jnp.where(core == 0, theirs, mine)], axis=0
        )
        squares = squares + jnp.sum(rows * rows)
        term = jnp.dot(
            weights,
            jnp.dot(rows, right_root, precision=lax.Precision.HIGH),
            precision=lax.Precision.HIGH,
        )
        shaped = term if shaped is None else shaped + term
    count = block_size * block_size
    graft = jnp.sqrt(squares / count + epsilon) / jnp.sqrt(jnp.mean(shaped * shaped) + epsilon)
    finished = (shaped * graft).astype(jnp.bfloat16)

    near = lax.dynamic_slice_in_dim(finished, y * half, half, 1)
    far = lax.dynamic_slice_in_dim(finished, (1 - y) * half, half, 1)
    far_parts = [far[:half], far[half:]]
    across = moved(near, across_x)
    beside = [moved(part, across_y) for part in far_parts]
    diagonal = [moved(part, across_x) for part in beside]
    depth = block_size // 2
    parts = [
        (near, x, y, 0),
        (beside[0], x, 1 - y, 0),
        (beside[1], x, 1 - y, depth),
        (across, 1 - x, y, 0),
        (diagonal[0], 1 - x, 1 - y, 0),
        (diagonal[1], 1 - x, 1 - y, depth),
    ]
    result = jnp.zeros((n_gx * 2 * block_size, half), jnp.bfloat16)
    for part, from_x, from_y, offset in parts:
        other = moved(part, across_cores)
        for block, from_core in ((part, core), (other, 1 - core)):
            row = (4 * from_x + 2 * from_core + from_y) * block_size + offset
            result = lax.dynamic_update_slice(result, block, (row, jnp.int32(0)))
    return result


def solution(mesh):
    in_specs = (
        P("gx", "gy"),
        P("gx", "gy"),
        P(("gx", "gy"), None, None),
        P(("gx", "gy"), None, None),
    )
    out_specs = P(None, "gy")

    n_gx, n_gy = mesh.shape["gx"], mesh.shape["gy"]
    paired = n_gx == 4 and n_gy == 2 * n_gx

    def local(activations, out_grads, left_roots, right_roots):
        if paired and activations.shape[1] == left_roots.shape[1]:
            return lined(activations, out_grads, left_roots, right_roots)
        return general(activations, out_grads, left_roots, right_roots)

    return jax.shard_map(local, mesh=mesh, in_specs=in_specs, out_specs=out_specs, check_vma=False)
```

```python
import jax
import jax.numpy as jnp
from jax import lax
from jax.experimental import pallas as pl
from jax.experimental.pallas import tpu as pltpu
from jax.sharding import PartitionSpec as P


epsilon = 1e-06
AXES = ("gx", "gy")
PARTS = (1, 1)
STRIPS = 4


def partner(block, axis, distance):
    count = lax.axis_size(axis)
    route = []
    for low in range(count):
        high = low | 1 << distance
        if high != low and high < count:
            route += [(low, high), (high, low)]
    return lax.ppermute(block, axis, route)


def general(activations, out_grads, left_roots, right_roots):
    block_size = left_roots.shape[1]
    half_width = block_size // 2
    parity = lax.axis_index("gy") % 2
    is_even = parity == 0
    gathered = lax.all_gather(activations, "gy", axis=1, tiled=True)
    summed = lax.psum_scatter(
        lax.dot_general(
            gathered, out_grads, (((0,), (0,)), ((), ())), preferred_element_type=jnp.float32
        ),
        "gx",
        scatter_dimension=0,
        tiled=True,
    )
    own_part = lax.dynamic_slice_in_dim(summed, parity * block_size, block_size, 0)
    far_part = lax.dynamic_slice_in_dim(summed, (1 - parity) * block_size, block_size, 0)
    received = partner(far_part, "gy", 0)
    left_block = jnp.where(is_even, own_part, received)
    right_block = jnp.where(is_even, received, own_part)
    grad_block = jnp.concatenate([left_block, right_block], axis=1)
    finished = precondition(grad_block, left_roots[0], right_roots[0])
    own_part = lax.dynamic_slice_in_dim(finished, parity * half_width, half_width, 1)
    far_part = lax.dynamic_slice_in_dim(finished, (1 - parity) * half_width, half_width, 1)
    received = partner(far_part, "gy", 0)
    upper_rows = jnp.where(is_even, own_part, received)
    lower_rows = jnp.where(is_even, received, own_part)
    paired = jnp.concatenate([upper_rows, lower_rows], axis=0)
    return lax.all_gather(paired, "gx", axis=0, tiled=True)


def precondition(grad_block, left_root, right_root):
    shaped = jnp.dot(
        jnp.dot(left_root, grad_block, precision=lax.Precision.HIGH),
        right_root,
        precision=lax.Precision.HIGH,
    )
    graft = jnp.sqrt(jnp.mean(grad_block * grad_block) + epsilon) / jnp.sqrt(
        jnp.mean(shaped * shaped) + epsilon
    )
    return (shaped * graft).astype(jnp.bfloat16)


def routes(n_gx, n_gy, target):
    found = []
    for gx in range(n_gx):
        for gy in range(n_gy):
            to = target(gx // 2, gx % 2, gy // 2, gy % 2)
            if to is not None:
                x, core, z, y = to
                found.append((gx * n_gy + gy, (2 * x + core) * n_gy + 2 * z + y))
    return found


def send(block, route):
    return lax.ppermute(block, AXES, route)


def in_vmem(count):
    return [pl.BlockSpec(memory_space=pltpu.VMEM)] * count


def params(mebibytes):
    return pltpu.CompilerParams(vmem_limit_bytes=mebibytes * 2**20)


def whereabouts():
    gx, gy = lax.axis_index("gx"), lax.axis_index("gy")
    return gx // 2, gx % 2, gy // 2, gy % 2


def transposed_product(choices, columns, pick):
    contracted, width = choices[0].shape
    count = columns.shape[1]

    def kernel(*refs):
        *choice_refs, columns_ref, out_ref, taken_ref = refs
        if len(choice_refs) == 1:
            taken_ref = choice_refs[0]
        else:
            index = pick(whereabouts()[2])

            def take(choice_ref):
                taken_ref[...] = choice_ref[...]

            for number, choice_ref in enumerate(choice_refs):
                pl.when(index == number)(lambda ref=choice_ref: take(ref))

        out_ref[...] = lax.dot_general(
            taken_ref[...],
            columns_ref[...],
            (((0,), (0,)), ((), ())),
            preferred_element_type=jnp.float32,
        )

    return pl.pallas_call(
        kernel,
        out_shape=jax.ShapeDtypeStruct((width, count), jnp.float32),
        in_specs=in_vmem(len(choices) + 1),
        out_specs=in_vmem(1)[0],
        scratch_shapes=[pltpu.VMEM((contracted, width), jnp.bfloat16)],
        cost_estimate=pl.CostEstimate(
            flops=2 * contracted * width * count,
            transcendentals=0,
            bytes_accessed=2 * contracted * (width + count) + 4 * width * count,
        ),
        compiler_params=params(16),
        name="token_product",
    )(*choices, columns)


def halves(value):
    high = value.astype(jnp.bfloat16)
    return high, (value - high.astype(jnp.float32)).astype(jnp.bfloat16)


def kept_halves(value):
    high = lax.reduce_precision(value, exponent_bits=8, mantissa_bits=7)
    return high.astype(jnp.bfloat16), (value - high).astype(jnp.bfloat16)


def three_pass(left, right):
    def single(a, b):
        return jnp.dot(a, b, preferred_element_type=jnp.float32)

    return single(left[0], right[0]) + (single(left[0], right[1]) + single(left[1], right[0]))


def advance(squares, sums, left, right, so_far, final, low, last):
    width = sums[0].shape[0]
    size = right[0].shape[0]
    half = size // 2
    strip = size // STRIPS
    given = 0 if so_far is None else 1

    def kernel(*refs):
        squares_ref, part, same, cross, mate, mine, theirs, lh, ll, rh, rl = refs[:11]
        acc = refs[11] if given else None
        outs, (shaped, rows) = refs[11 + given : -2], refs[-2:]
        if not last:
            shaped = outs[0]
        x, core, z, y = whereabouts()
        is_last = chosen(final, z) == 2 * x + core
        my_rows = jnp.where(is_last, part[...] + same[...], mine[...])
        their_rows = jnp.where(is_last, cross[...] + mate[...], theirs[...])
        rows[:width] = jnp.where(core == 0, my_rows, their_rows)
        rows[width:] = jnp.where(core == 0, their_rows, my_rows)
        entry = squares_ref[0] + jnp.sum(my_rows * my_rows) + jnp.sum(their_rows * their_rows)
        piece = halves(rows[...])

        inner = halves(three_pass(piece, (rh[...], rl[...])))

        def second(number, total):
            at = pl.ds(pl.multiple_of(number * strip, strip), strip)

            def weights(ref):
                return jnp.concatenate(
                    [ref[at, low : low + width], ref[at, half + low : half + low + width]], axis=1
                )

            block = three_pass((weights(lh), weights(ll)), inner)
            if given:
                block = acc[at] + block
            shaped[at] = block
            return total + jnp.sum(block * block) if last else total

        result = lax.fori_loop(0, STRIPS, second, jnp.float32(0), unroll=True)
        if not last:
            outs[1][0] = entry
            return
        near, far_0, far_1 = outs
        count = size * size
        graft = jnp.sqrt(entry / count + epsilon) / jnp.sqrt(result / count + epsilon)

        def store(near_columns, far_columns):
            near[...] = (shaped[:, near_columns] * graft).astype(jnp.bfloat16)
            far_0[...] = (shaped[:half, far_columns] * graft).astype(jnp.bfloat16)
            far_1[...] = (shaped[half:, far_columns] * graft).astype(jnp.bfloat16)

        one, other = pl.ds(0, half), pl.ds(half, half)
        pl.when(y == 0)(lambda: store(one, other))
        pl.when(y == 1)(lambda: store(other, one))

    smem = pl.BlockSpec(memory_space=pltpu.SMEM)
    if last:
        out_shape = [
            jax.ShapeDtypeStruct((size, half), jnp.bfloat16),
            jax.ShapeDtypeStruct((half, half), jnp.bfloat16),
            jax.ShapeDtypeStruct((half, half), jnp.bfloat16),
        ]
        out_specs = in_vmem(3)
    else:
        out_shape = [
            jax.ShapeDtypeStruct((size, size), jnp.float32),
            jax.ShapeDtypeStruct((1,), jnp.float32),
        ]
        out_specs = in_vmem(1) + [smem]
    scratch_size = size if last else 8
    return pl.pallas_call(
        kernel,
        out_shape=out_shape,
        in_specs=[smem] + in_vmem(10 + given),
        out_specs=out_specs,
        input_output_aliases={11: 0} if given and not last else {},
        scratch_shapes=[
            pltpu.VMEM((scratch_size, size), jnp.float32),
            pltpu.VMEM((2 * width, size), jnp.float32),
        ],
        cost_estimate=pl.CostEstimate(
            flops=24 * width * size * size, transcendentals=0, bytes_accessed=20 * size * size
        ),
        compiler_params=params(24 if last else 16),
        name="finish" if last else "advance",
    )(squares, *sums, *left, *right, *([so_far] if given else []))


def chosen(table, z):
    value = jnp.int32(table[0])
    for position in range(1, len(table)):
        value = jnp.where(z == position, jnp.int32(table[position]), value)
    return value


def lined(activations, out_grads, left_roots, right_roots):
    n_gx, n_gy = lax.axis_size("gx"), lax.axis_size("gy")
    n_z = n_gy // 2
    gx, gy = lax.axis_index("gx"), lax.axis_index("gy")
    x, core, z, y = gx // 2, gx % 2, gy // 2, gy % 2
    block_size = left_roots.shape[1]
    half = block_size // 2
    widths = [half * part // sum(PARTS) for part in PARTS]
    starts = [sum(widths[:h]) for h in range(len(widths))]
    pieces = range(len(widths))
    left_root, right_root = left_roots[0], right_roots[0]

    def route(target):
        return routes(n_gx, n_gy, target)

    across_x = route(lambda x, c, z, y: (1 - x, c, z, y))
    across_y = route(lambda x, c, z, y: (x, c, z, 1 - y))
    across_xy = route(lambda x, c, z, y: (1 - x, c, z, 1 - y))
    across_cores = route(lambda x, c, z, y: (x, 1 - c, z, y))

    def moved(block, path):
        return send(block, path)

    own = []
    for h in pieces:
        near = lax.dynamic_slice_in_dim(activations, core * half + starts[h], widths[h], 1)
        far = lax.dynamic_slice_in_dim(
            activations, (1 - core) * half + starts[h], widths[h], 1
        )
        swapped = moved(far, across_cores)
        own.append(jnp.concatenate([near, swapped], axis=0))

    up_1 = route(lambda x, c, z, y: (x, c, z + 1, y) if z < n_z - 1 else None)
    down_1 = route(lambda x, c, z, y: (x, c, z - 1, y) if z > 0 else None)
    up_2 = route(lambda x, c, z, y: (x, c, z + 1, y) if 0 < z < n_z - 1 else None)
    down_2 = route(lambda x, c, z, y: (x, c, z - 1, y) if 0 < z < n_z - 1 else None)
    ends = route(
        lambda x, c, z, y: (x, c, z + 1, y) if z == n_z - 2 else ((x, c, z - 1, y) if z == 1 else None)
    )
    is_upper = z >= n_z // 2
    first_up = [moved(own[h], up_1) for h in pieces]
    first_down = [moved(own[h], down_1) for h in pieces]
    second_up = [moved(first_up[h], up_2) for h in pieces]
    second_down = [moved(first_down[h], down_2) for h in pieces]
    second = [jnp.where(is_upper, u, d) for u, d in zip(second_up, second_down)]
    third = [moved(second[h], ends) for h in pieces]

    other_half = moved(out_grads, across_y)
    columns = jnp.where(
        y == 0,
        jnp.concatenate([out_grads, other_half], axis=1),
        jnp.concatenate([other_half, out_grads], axis=1),
    )
    columns = jnp.concatenate([columns, moved(columns, across_cores)], axis=0)

    def partial_sum(step, h):
        def lower(z):
            return z < n_z // 2

        def at_end(z):
            return (z == 0) | (z == n_z - 1)

        if step == 0:
            return transposed_product([own[h]], columns, None)
        if step == 1:
            return transposed_product(
                [first_up[h], first_down[h]], columns, lambda z: jnp.where(lower(z), 1, 0)
            )
        if step == 2:
            return transposed_product(
                [second[h], first_up[h], first_down[h]],
                columns,
                lambda z: jnp.where(at_end(z), 0, jnp.where(lower(z), 1, 2)),
            )
        return transposed_product(
            [third[h], second[h]], columns, lambda z: jnp.where(at_end(z), 0, 1)
        )

    tables = [[0, 1, 2, 3], [1, 2, 1, 2], [2, 0, 3, 1], [3, 3, 0, 0]]
    sources = [chosen(table, z) for table in tables]
    final = tables[-1]
    same_core = route(
        lambda x, c, z, y: (1 - x, c, z, y)
        if (x, c) == (1 - final[z] // 2, final[z] % 2)
        else None
    )
    cross_core = route(
        lambda x, c, z, y: (1 - x, 1 - c, z, y)
        if (x, c) == (1 - final[z] // 2, 1 - final[z] % 2)
        else None
    )
    chip_mate = route(
        lambda x, c, z, y: (x, 1 - c, z, y)
        if (x, c) == (final[z] // 2, 1 - final[z] % 2)
        else None
    )
    shaped = None
    squares = jnp.zeros((1,), jnp.float32)
    left, right = kept_halves(left_root), kept_halves(right_root)
    for h in pieces:
        mine = theirs = None
        for step in range(3):
            part = partial_sum(step, h)
            table = tables[step]

            def to_owner(x, c, z, y):
                owner = table[z] // 2
                return (owner, c, z, y) if x != owner else None

            crossed = moved(part, route(to_owner))
            total = part + crossed
            if mine is None:
                mine, theirs = total, total
            else:
                mine = jnp.where(sources[step] == gx, total, mine)
                theirs = jnp.where(sources[step] == 2 * x + 1 - core, total, theirs)
        mine, theirs = lax.optimization_barrier((mine, theirs))
        theirs = moved(theirs, across_cores)
        part = partial_sum(3, h)
        from_same = moved(part, same_core)
        from_cross = moved(part, cross_core)
        from_mate = moved(part, chip_mate)
        final_piece = h == len(widths) - 1
        outcome = advance(
            squares,
            (part, from_same, from_cross, from_mate, mine, theirs),
            left,
            right,
            shaped,
            final,
            starts[h],
            final_piece,
        )
        if not final_piece:
            shaped, squares = outcome
    near, *far_parts = outcome

    across = moved(near, across_x)
    beside = [moved(part, across_y) for part in far_parts]
    diagonal = [moved(part, across_x) for part in beside]
    depth = block_size // 2
    parts = [
        (near, x, y, 0),
        (beside[0], x, 1 - y, 0),
        (beside[1], x, 1 - y, depth),
        (across, 1 - x, y, 0),
        (diagonal[0], 1 - x, 1 - y, 0),
        (diagonal[1], 1 - x, 1 - y, depth),
    ]
    result = jnp.zeros((n_gx * 2 * block_size, half), jnp.bfloat16)
    for part, from_x, from_y, offset in parts:
        other = moved(part, across_cores)
        for block, from_core in ((part, core), (other, 1 - core)):
            row = (4 * from_x + 2 * from_core + from_y) * block_size + offset
            result = lax.dynamic_update_slice(result, block, (row, jnp.int32(0)))
    return result


def solution(mesh):
    in_specs = (
        P("gx", "gy"),
        P("gx", "gy"),
        P(("gx", "gy"), None, None),
        P(("gx", "gy"), None, None),
    )
    out_specs = P(None, "gy")

    n_gx, n_gy = mesh.shape["gx"], mesh.shape["gy"]
    paired = n_gx == 4 and n_gy == 2 * n_gx

    def local(activations, out_grads, left_roots, right_roots):
        if paired and activations.shape[1] == left_roots.shape[1]:
            return lined(activations, out_grads, left_roots, right_roots)
        return general(activations, out_grads, left_roots, right_roots)

    return jax.shard_map(local, mesh=mesh, in_specs=in_specs, out_specs=out_specs, check_vma=False)
```

```python
import jax
import jax.numpy as jnp
from jax import lax
from jax.experimental import pallas as pl
from jax.experimental.pallas import tpu as pltpu
from jax.sharding import PartitionSpec as P


epsilon = 1e-06
AXES = ("gx", "gy")
PARTS = (1, 1)
STRIPS = 4


def partner(block, axis, distance):
    count = lax.axis_size(axis)
    route = []
    for low in range(count):
        high = low | 1 << distance
        if high != low and high < count:
            route += [(low, high), (high, low)]
    return lax.ppermute(block, axis, route)


def general(activations, out_grads, left_roots, right_roots):
    block_size = left_roots.shape[1]
    half_width = block_size // 2
    parity = lax.axis_index("gy") % 2
    is_even = parity == 0
    gathered = lax.all_gather(activations, "gy", axis=1, tiled=True)
    summed = lax.psum_scatter(
        lax.dot_general(
            gathered, out_grads, (((0,), (0,)), ((), ())), preferred_element_type=jnp.float32
        ),
        "gx",
        scatter_dimension=0,
        tiled=True,
    )
    own_part = lax.dynamic_slice_in_dim(summed, parity * block_size, block_size, 0)
    far_part = lax.dynamic_slice_in_dim(summed, (1 - parity) * block_size, block_size, 0)
    received = partner(far_part, "gy", 0)
    left_block = jnp.where(is_even, own_part, received)
    right_block = jnp.where(is_even, received, own_part)
    grad_block = jnp.concatenate([left_block, right_block], axis=1)
    finished = precondition(grad_block, left_roots[0], right_roots[0])
    own_part = lax.dynamic_slice_in_dim(finished, parity * half_width, half_width, 1)
    far_part = lax.dynamic_slice_in_dim(finished, (1 - parity) * half_width, half_width, 1)
    received = partner(far_part, "gy", 0)
    upper_rows = jnp.where(is_even, own_part, received)
    lower_rows = jnp.where(is_even, received, own_part)
    paired = jnp.concatenate([upper_rows, lower_rows], axis=0)
    return lax.all_gather(paired, "gx", axis=0, tiled=True)


def precondition(grad_block, left_root, right_root):
    shaped = jnp.dot(
        jnp.dot(left_root, grad_block, precision=lax.Precision.HIGH),
        right_root,
        precision=lax.Precision.HIGH,
    )
    graft = jnp.sqrt(jnp.mean(grad_block * grad_block) + epsilon) / jnp.sqrt(
        jnp.mean(shaped * shaped) + epsilon
    )
    return (shaped * graft).astype(jnp.bfloat16)


def routes(n_gx, n_gy, target):
    found = []
    for gx in range(n_gx):
        for gy in range(n_gy):
            to = target(gx // 2, gx % 2, gy // 2, gy % 2)
            if to is not None:
                x, core, z, y = to
                found.append((gx * n_gy + gy, (2 * x + core) * n_gy + 2 * z + y))
    return found


def send(block, route):
    return lax.ppermute(block, AXES, route)


def in_vmem(count):
    return [pl.BlockSpec(memory_space=pltpu.VMEM)] * count


def params(mebibytes):
    return pltpu.CompilerParams(vmem_limit_bytes=mebibytes * 2**20)


def whereabouts():
    gx, gy = lax.axis_index("gx"), lax.axis_index("gy")
    return gx // 2, gx % 2, gy // 2, gy % 2


def transposed_product(choices, columns, pick, strips):
    contracted, width = choices[0].shape
    count = columns.shape[1]

    def kernel(*refs):
        *choice_refs, columns_ref, out_ref, taken_ref = refs
        if len(choice_refs) == 1:
            taken_ref = choice_refs[0]
        else:
            index = pick(whereabouts()[2])

            def take(choice_ref):
                taken_ref[...] = choice_ref[...]

            for number, choice_ref in enumerate(choice_refs):
                pl.when(index == number)(lambda ref=choice_ref: take(ref))

        strip = count // strips

        def step(number, carry):
            at = pl.ds(pl.multiple_of(number * strip, strip), strip)
            out_ref[:, at] = lax.dot_general(
                taken_ref[...],
                columns_ref[:, at],
                (((0,), (0,)), ((), ())),
                preferred_element_type=jnp.float32,
            )
            return carry

        lax.fori_loop(0, strips, step, 0, unroll=strips == 1)

    return pl.pallas_call(
        kernel,
        out_shape=jax.ShapeDtypeStruct((width, count), jnp.float32),
        in_specs=in_vmem(len(choices) + 1),
        out_specs=in_vmem(1)[0],
        scratch_shapes=[pltpu.VMEM((contracted, width), jnp.bfloat16)],
        cost_estimate=pl.CostEstimate(
            flops=2 * contracted * width * count,
            transcendentals=0,
            bytes_accessed=2 * contracted * (width + count) + 4 * width * count,
        ),
        compiler_params=params(16),
        name="token_product",
    )(*choices, columns)


def halves(value):
    high = value.astype(jnp.bfloat16)
    return high, (value - high.astype(jnp.float32)).astype(jnp.bfloat16)


def kept_halves(value):
    high = lax.reduce_precision(value, exponent_bits=8, mantissa_bits=7)
    return high.astype(jnp.bfloat16), (value - high).astype(jnp.bfloat16)


def three_pass(left, right):
    def single(a, b):
        return jnp.dot(a, b, preferred_element_type=jnp.float32)

    return single(left[0], right[0]) + (single(left[0], right[1]) + single(left[1], right[0]))


def advance(squares, sums, left, right, so_far, final, low, outputs):
    width = sums[0].shape[0]
    size = right[0].shape[0]
    half = size // 2
    strip = size // STRIPS
    given = 0 if so_far is None else 1
    late = len(sums) > 2
    unrolled = outputs > 0 or late

    def kernel(squares_ref, *refs):
        sum_refs, refs = refs[: len(sums)], refs[len(sums) :]
        (lh, ll, rh, rl), refs = refs[:4], refs[4:]
        acc, refs = (refs[0], refs[1:]) if given else (None, refs)
        outs, (shaped, rows, inner_high, inner_low) = refs[:-4], refs[-4:]
        if not outputs:
            shaped = outs[0]
        x, core, z, y = whereabouts()
        my_rows, their_rows = sum_refs[0][...], sum_refs[1][...]
        if late:
            part, same, cross, mate = sum_refs[2:]
            is_last = chosen(final, z) == 2 * x + core
            my_rows = jnp.where(is_last, part[...] + same[...], my_rows)
            their_rows = jnp.where(is_last, cross[...] + mate[...], their_rows)
        rows[:width] = jnp.where(core == 0, my_rows, their_rows)
        rows[width:] = jnp.where(core == 0, their_rows, my_rows)
        entry = squares_ref[0] + jnp.sum(my_rows * my_rows) + jnp.sum(their_rows * their_rows)
        piece = halves(rows[...])
        if unrolled:
            inner_high[...], inner_low[...] = halves(three_pass(piece, (rh[...], rl[...])))
        else:

            def first(number, carry):
                at = pl.ds(pl.multiple_of(number * strip, strip), strip)
                high, low = halves(three_pass(piece, (rh[:, at], rl[:, at])))
                inner_high[:, at] = high
                inner_low[:, at] = low
                return carry

            lax.fori_loop(0, STRIPS, first, 0)
        inner = inner_high[...], inner_low[...]

        def second(number, total):
            at = pl.ds(pl.multiple_of(number * strip, strip), strip)

            def weights(ref):
                return jnp.concatenate(
                    [ref[at, low : low + width], ref[at, half + low : half + low + width]], axis=1
                )

            block = three_pass((weights(lh), weights(ll)), inner)
            if given:
                block = acc[at] + block
            shaped[at] = block
            return total + jnp.sum(block * block) if outputs else total

        result = lax.fori_loop(0, STRIPS, second, jnp.float32(0), unroll=unrolled)
        if not outputs:
            outs[1][0] = entry
            return
        count = size * size
        graft = jnp.sqrt(entry / count + epsilon) / jnp.sqrt(result / count + epsilon)

        def store(near_columns, far_columns):
            outs[0][...] = (shaped[:, near_columns] * graft).astype(jnp.bfloat16)
            if outputs == 3:
                outs[1][...] = (shaped[:half, far_columns] * graft).astype(jnp.bfloat16)
                outs[2][...] = (shaped[half:, far_columns] * graft).astype(jnp.bfloat16)

        one, other = pl.ds(0, half), pl.ds(half, half)
        pl.when(y == 0)(lambda: store(one, other))
        pl.when(y == 1)(lambda: store(other, one))

    smem = pl.BlockSpec(memory_space=pltpu.SMEM)
    if outputs:
        shapes = [(size, half), (half, half), (half, half)][:outputs]
        out_shape = [jax.ShapeDtypeStruct(shape, jnp.bfloat16) for shape in shapes]
        out_specs = in_vmem(outputs)
    else:
        out_shape = [
            jax.ShapeDtypeStruct((size, size), jnp.float32),
            jax.ShapeDtypeStruct((1,), jnp.float32),
        ]
        out_specs = in_vmem(1) + [smem]
    return pl.pallas_call(
        kernel,
        out_shape=out_shape,
        in_specs=[smem] + in_vmem(len(sums) + 4 + given),
        out_specs=out_specs,
        scratch_shapes=[
            pltpu.VMEM((size if outputs else 8, size), jnp.float32),
            pltpu.VMEM((2 * width, size), jnp.float32),
            pltpu.VMEM((2 * width, size), jnp.bfloat16),
            pltpu.VMEM((2 * width, size), jnp.bfloat16),
        ],
        cost_estimate=pl.CostEstimate(
            flops=24 * width * size * size, transcendentals=0, bytes_accessed=20 * size * size
        ),
        compiler_params=params(24 if outputs else 16),
        name="finish" if outputs else "advance",
    )(squares, *sums, *left, *right, *([so_far] if given else []))


def put(result, blocks, places, height, block_size):
    width = blocks[0].shape[1]
    given = 0 if result is None else 1

    def kernel(*refs):
        block_refs, out_ref, sems = refs[: len(blocks)], refs[-2], refs[-1]
        x, core, _, y = whereabouts()
        copies = []
        for number, (ref, (dx, dc, dy, offset)) in enumerate(zip(block_refs, places)):
            from_x = 1 - x if dx else x
            from_core = 1 - core if dc else core
            from_y = 1 - y if dy else y
            row = (4 * from_x + 2 * from_core + from_y) * block_size + offset
            row = pl.multiple_of(row, block_size // 2)
            target = out_ref.at[pl.ds(row, ref.shape[0])]
            copies.append(pltpu.make_async_copy(ref, target, sems.at[number]))
        for copy in copies:
            copy.start()
        for copy in copies:
            copy.wait()

    anywhere = pl.BlockSpec(memory_space=pl.ANY)
    return pl.pallas_call(
        kernel,
        out_shape=jax.ShapeDtypeStruct((height, width), blocks[0].dtype),
        in_specs=in_vmem(len(blocks)) + [anywhere] * given,
        out_specs=anywhere,
        scratch_shapes=[pltpu.SemaphoreType.DMA((len(blocks),))],
        input_output_aliases={len(blocks): 0} if given else {},
        cost_estimate=pl.CostEstimate(
            flops=2 * sum(block.size for block in blocks) * 256,
            transcendentals=0,
            bytes_accessed=4 * sum(block.size for block in blocks),
        ),
        compiler_params=params(16),
        name="put",
    )(*blocks, *([result] if given else []))


def chosen(table, z):
    value = jnp.int32(table[0])
    for position in range(1, len(table)):
        value = jnp.where(z == position, jnp.int32(table[position]), value)
    return value


def lined(activations, out_grads, left_roots, right_roots):
    n_gx, n_gy = lax.axis_size("gx"), lax.axis_size("gy")
    n_z = n_gy // 2
    gx, gy = lax.axis_index("gx"), lax.axis_index("gy")
    x, core, z, y = gx // 2, gx % 2, gy // 2, gy % 2
    block_size = left_roots.shape[1]
    half = block_size // 2
    widths = [half * part // sum(PARTS) for part in PARTS]
    starts = [sum(widths[:h]) for h in range(len(widths))]
    pieces = range(len(widths))
    left_root, right_root = left_roots[0], right_roots[0]

    def route(target):
        return routes(n_gx, n_gy, target)

    across_x = route(lambda x, c, z, y: (1 - x, c, z, y))
    across_y = route(lambda x, c, z, y: (x, c, z, 1 - y))
    across_xy = route(lambda x, c, z, y: (1 - x, c, z, 1 - y))
    across_cores = route(lambda x, c, z, y: (x, 1 - c, z, y))

    def moved(block, path):
        return send(block, path)

    own = []
    for h in pieces:
        near = lax.dynamic_slice_in_dim(activations, core * half + starts[h], widths[h], 1)
        far = lax.dynamic_slice_in_dim(
            activations, (1 - core) * half + starts[h], widths[h], 1
        )
        swapped = moved(far, across_cores)
        own.append(jnp.concatenate([near, swapped], axis=0))

    up_1 = route(lambda x, c, z, y: (x, c, z + 1, y) if z < n_z - 1 else None)
    down_1 = route(lambda x, c, z, y: (x, c, z - 1, y) if z > 0 else None)
    up_2 = route(lambda x, c, z, y: (x, c, z + 1, y) if 0 < z < n_z - 1 else None)
    down_2 = route(lambda x, c, z, y: (x, c, z - 1, y) if 0 < z < n_z - 1 else None)
    ends = route(
        lambda x, c, z, y: (x, c, z + 1, y) if z == n_z - 2 else ((x, c, z - 1, y) if z == 1 else None)
    )
    is_upper = z >= n_z // 2
    first_up = [moved(own[h], up_1) for h in pieces]
    first_down = [moved(own[h], down_1) for h in pieces]
    second_up = [moved(first_up[h], up_2) for h in pieces]
    second_down = [moved(first_down[h], down_2) for h in pieces]
    second = [jnp.where(is_upper, u, d) for u, d in zip(second_up, second_down)]
    third = [moved(second[h], ends) for h in pieces]

    other_half = moved(out_grads, across_y)
    columns = jnp.where(
        y == 0,
        jnp.concatenate([out_grads, other_half], axis=1),
        jnp.concatenate([other_half, out_grads], axis=1),
    )
    columns = jnp.concatenate([columns, moved(columns, across_cores)], axis=0)

    def partial_sum(step, h):
        def lower(z):
            return z < n_z // 2

        def at_end(z):
            return (z == 0) | (z == n_z - 1)

        if step == 0:
            return transposed_product([own[h]], columns, None, STRIPS)
        if step == 1:
            return transposed_product(
                [first_up[h], first_down[h]],
                columns,
                lambda z: jnp.where(lower(z), 1, 0),
                STRIPS,
            )
        if step == 2:
            return transposed_product(
                [second[h], first_up[h], first_down[h]],
                columns,
                lambda z: jnp.where(at_end(z), 0, jnp.where(lower(z), 1, 2)),
                STRIPS,
            )
        return transposed_product(
            [third[h], second[h]], columns, lambda z: jnp.where(at_end(z), 0, 1), 1
        )

    tables = [[0, 1, 2, 3], [1, 2, 1, 2], [2, 0, 3, 1], [3, 3, 0, 0]]
    sources = [chosen(table, z) for table in tables]
    final = tables[-1]
    same_core = route(
        lambda x, c, z, y: (1 - x, c, z, y)
        if (x, c) == (1 - final[z] // 2, final[z] % 2)
        else None
    )
    cross_core = route(
        lambda x, c, z, y: (1 - x, 1 - c, z, y)
        if (x, c) == (1 - final[z] // 2, 1 - final[z] % 2)
        else None
    )
    chip_mate = route(
        lambda x, c, z, y: (x, 1 - c, z, y)
        if (x, c) == (final[z] // 2, 1 - final[z] % 2)
        else None
    )
    shaped = None
    squares = early_squares = jnp.zeros((1,), jnp.float32)
    early_shaped = None
    left, right = kept_halves(left_root), kept_halves(right_root)
    for h in pieces:
        mine = theirs = None
        for step in range(3):
            part = partial_sum(step, h)
            table = tables[step]

            def to_owner(x, c, z, y):
                owner = table[z] // 2
                return (owner, c, z, y) if x != owner else None

            crossed = moved(part, route(to_owner))
            total = part + crossed
            if mine is None:
                mine, theirs = total, total
            else:
                mine = jnp.where(sources[step] == gx, total, mine)
                theirs = jnp.where(sources[step] == 2 * x + 1 - core, total, theirs)
        mine, theirs = lax.optimization_barrier((mine, theirs))
        theirs = moved(theirs, across_cores)
        final_piece = h == len(widths) - 1
        early = advance(
            early_squares,
            (mine, theirs),
            left,
            right,
            early_shaped,
            final,
            starts[h],
            1 if final_piece else 0,
        )
        if not final_piece:
            early_shaped, early_squares = early
        part = partial_sum(3, h)
        from_same = moved(part, same_core)
        from_cross = moved(part, cross_core)
        from_mate = moved(part, chip_mate)
        outcome = advance(
            squares,
            (mine, theirs, part, from_same, from_cross, from_mate),
            left,
            right,
            shaped,
            final,
            starts[h],
            3 if final_piece else 0,
        )
        if not final_piece:
            shaped, squares = outcome
    near, *far_parts = outcome

    early_route = route(lambda x, c, z, y: (1 - x, c, z, y) if 2 * x + c != final[z] else None)
    late_route = route(lambda x, c, z, y: (1 - x, c, z, y) if 2 * x + c == final[z] else None)
    across = jnp.where(
        sources[3] == 2 * (1 - x) + core, moved(near, late_route), moved(early[0], early_route)
    )
    beside = [moved(part, across_y) for part in far_parts]
    diagonal = [moved(part, across_x) for part in beside]
    depth = block_size // 2
    parts = [
        (near, 0, 0, 0),
        (beside[0], 0, 1, 0),
        (beside[1], 0, 1, depth),
        (across, 1, 0, 0),
        (diagonal[0], 1, 1, 0),
        (diagonal[1], 1, 1, depth),
    ]
    others = [moved(part, across_cores) for part, *_ in parts]
    result = None
    for members in ((0, 1, 2, 3), (4,), (5,)):
        blocks, places = [], []
        for member in members:
            part, dx, dy, offset = parts[member]
            blocks += [part, others[member]]
            places += [(dx, 0, dy, offset), (dx, 1, dy, offset)]
        result = put(result, blocks, places, n_gx * 2 * block_size, block_size)
    return result


def solution(mesh):
    in_specs = (
        P("gx", "gy"),
        P("gx", "gy"),
        P(("gx", "gy"), None, None),
        P(("gx", "gy"), None, None),
    )
    out_specs = P(None, "gy")

    n_gx, n_gy = mesh.shape["gx"], mesh.shape["gy"]
    paired = n_gx == 4 and n_gy == 2 * n_gx

    def local(activations, out_grads, left_roots, right_roots):
        if paired and activations.shape[1] == left_roots.shape[1]:
            return lined(activations, out_grads, left_roots, right_roots)
        return general(activations, out_grads, left_roots, right_roots)

    return jax.shard_map(local, mesh=mesh, in_specs=in_specs, out_specs=out_specs, check_vma=False)
```
